32 devices in a mesh: dp: 1 (over z), gp: 32 (over y, x, core).
Axes of the slice: x: 4, y: 4, z: 1, core: 2. Of those that a mesh axis runs over, the one named last changes fastest.
The devices are a block of a 4x4x8 slice.
Arguments:
- x_prev: float32 [16384, 83], P(('dp', 'gp'))
- x_cur: float32 [16384, 83], P(('dp', 'gp'))
- forcing: float32 [16384, 2, 5], P(('dp', 'gp'))
- grid_static: float32 [16384, 5], P(('dp', 'gp'))
- g2m_feat: float32 [16384, 4], P(('dp', 'gp'))
- m2g_feat: float32 [16384, 4], P(('dp', 'gp'))
- mesh_feat: float32 [4096, 3], P(('dp', 'gp'))
- mesh_edge_feat: float32 [4096, 6, 4], P(('dp', 'gp'))
- norm_stats: float32 [4, 83], replicated
- w_grid_in: bfloat16 [176, 512], replicated
- w_mesh_in: bfloat16 [3, 512], replicated
- w_eemb_in: bfloat16 [3, 4, 512], replicated
- w_embed_out: bfloat16 [5, 512, 512], replicated
- w_edge_in: bfloat16 [18, 1536, 512], replicated
- w_edge_out: bfloat16 [18, 512, 512], replicated
- w_node_in: bfloat16 [18, 1024, 512], replicated
- w_node_out: bfloat16 [18, 512, 512], replicated
- w_grid_self: bfloat16 [2, 512, 512], replicated
- w_out_hidden: bfloat16 [512, 512], replicated
- w_out_final: bfloat16 [512, 83], replicated
Outputs:
- output 1: float32 [16384, 83], P(('dp', 'gp'))
- output 2: float32 [16384, 83], P(('dp', 'gp'))
All inputs are finite; a program needn't handle non-finite values.
Results may differ from the reference program's by a relative error of at most 0.00836121.
Values are sent between devices in bfloat16 or wider.
A program may use at most 768 MiB of HBM per device.

```python
import jax
import jax.numpy as jnp
from jax import lax

GRID_NODES = 16384
MESH_NODES = 4096
SHIFT = 64
LATENT = 512
VARS = 83
FORCE = 5
STATIC = 5
LAYERS = 16
EDGE_FEAT = 4
MESH_FEAT = 3
OFFSET_COUNT = 6

GRID_RATIO = GRID_NODES // MESH_NODES
QUARTER = MESH_NODES // 4
BLOCKS = LAYERS + 2
IN_FEAT = 2 * VARS + FORCE + STATIC
OFFSETS = (1, -1, SHIFT, -SHIFT, QUARTER, -QUARTER)


def normal_weight(key_in, out_shape, fan_in):
    return (jax.random.normal(key_in, out_shape, jnp.float32) * fan_in ** -0.5).astype(jnp.bfloat16)


def setup_inputs(seed: int = 0, part: int = 0) -> dict:
    root_key = jax.random.key(seed)
    part_keys = jax.random.split(jax.random.fold_in(root_key, part), 8)
    weight_keys = jax.random.split(jax.random.key(seed + 1), 15)
    norm_stats = jnp.stack([
        0.5 * jax.random.normal(weight_keys[0], (VARS,), jnp.float32),
        jax.random.uniform(weight_keys[1], (VARS,), jnp.float32, 0.5, 1.5),
        0.2 * jax.random.normal(weight_keys[2], (VARS,), jnp.float32),
        jax.random.uniform(weight_keys[3], (VARS,), jnp.float32, 0.2, 0.6)])
    return {
        "x_prev": jax.random.normal(part_keys[0], (GRID_NODES, VARS), jnp.float32),
        "x_cur": jax.random.normal(part_keys[1], (GRID_NODES, VARS), jnp.float32),
        "forcing": jax.random.normal(part_keys[2], (GRID_NODES, 2, FORCE), jnp.float32),
        "grid_static": jax.random.normal(part_keys[3], (GRID_NODES, STATIC), jnp.float32),
        "g2m_feat": jax.random.normal(part_keys[4], (GRID_NODES, EDGE_FEAT), jnp.float32),
        "m2g_feat": jax.random.normal(part_keys[5], (GRID_NODES, EDGE_FEAT), jnp.float32),
        "mesh_feat": jax.random.normal(part_keys[6], (MESH_NODES, MESH_FEAT), jnp.float32),
        "mesh_edge_feat": jax.random.normal(part_keys[7], (MESH_NODES, OFFSET_COUNT, EDGE_FEAT), jnp.float32),
        "norm_stats": norm_stats,
        "w_grid_in": normal_weight(weight_keys[4], (IN_FEAT, LATENT), IN_FEAT),
        "w_mesh_in": normal_weight(weight_keys[5], (MESH_FEAT, LATENT), MESH_FEAT),
        "w_eemb_in": normal_weight(weight_keys[6], (3, EDGE_FEAT, LATENT), EDGE_FEAT),
        "w_embed_out": normal_weight(weight_keys[7], (5, LATENT, LATENT), LATENT),
        "w_edge_in": normal_weight(weight_keys[8], (BLOCKS, 3 * LATENT, LATENT), 3 * LATENT),
        "w_edge_out": normal_weight(weight_keys[9], (BLOCKS, LATENT, LATENT), LATENT),
        "w_node_in": normal_weight(weight_keys[10], (BLOCKS, 2 * LATENT, LATENT), 2 * LATENT),
        "w_node_out": normal_weight(weight_keys[11], (BLOCKS, LATENT, LATENT), LATENT),
        "w_grid_self": normal_weight(weight_keys[12], (2, LATENT, LATENT), LATENT),
        "w_out_hidden": normal_weight(weight_keys[13], (LATENT, LATENT), LATENT),
        "w_out_final": normal_weight(weight_keys[14], (LATENT, VARS), LATENT),
    }


def layer_norm(values):
    centre = jnp.mean(values, axis=-1, keepdims=True)
    centred = values - centre
    spread = jnp.mean(centred * centred, axis=-1, keepdims=True)
    return centred * lax.rsqrt(spread + 1e-5)


def matmul_f32(values, weight):
    return jnp.dot(values, weight, preferred_element_type=jnp.float32)


def mlp_tail(pre_act, w_second):
    hidden = jax.nn.silu(pre_act).astype(jnp.bfloat16)
    return layer_norm(matmul_f32(hidden, w_second))


def residual(base, update):
    return (base.astype(jnp.float32) + update).astype(jnp.bfloat16)


def embed_static(features, w_first, w_second):
    return mlp_tail(matmul_f32(features.astype(jnp.bfloat16), w_first), w_second).astype(jnp.bfloat16)


def reference(x_prev, x_cur, forcing, grid_static, g2m_feat, m2g_feat, mesh_feat, mesh_edge_feat, norm_stats, w_grid_in, w_mesh_in, w_eemb_in, w_embed_out, w_edge_in, w_edge_out, w_node_in, w_node_out, w_grid_self, w_out_hidden, w_out_final):
    mesh_lat = embed_static(mesh_feat, w_mesh_in, w_embed_out[1])
    g2m_lat = embed_static(g2m_feat, w_eemb_in[0], w_embed_out[2])
    m2g_lat = embed_static(m2g_feat, w_eemb_in[1], w_embed_out[3])
    edge_base = embed_static(mesh_edge_feat.reshape(MESH_NODES * OFFSET_COUNT, EDGE_FEAT), w_eemb_in[2], w_embed_out[4])
    in_mean = norm_stats[0]
    in_std = norm_stats[1]
    diff_mean = norm_stats[2]
    diff_std = norm_stats[3]

    def proc_layer(layer_state, layer_weights):
        mesh_cur, edge_lat = layer_state
        w_edge, w_edge_two, w_node, w_node_two = layer_weights
        send_proj = matmul_f32(mesh_cur, w_edge[LATENT:2 * LATENT])
        send_term = jnp.stack([jnp.roll(send_proj, -offset, axis=0) for offset in OFFSETS], axis=1).reshape(MESH_NODES * OFFSET_COUNT, LATENT)
        recv_term = matmul_f32(mesh_cur, w_edge[2 * LATENT:])
        pre_act = matmul_f32(edge_lat, w_edge[:LATENT]) + send_term
        pre_act = (pre_act.reshape(MESH_NODES, OFFSET_COUNT, LATENT) + recv_term[:, None, :]).reshape(MESH_NODES * OFFSET_COUNT, LATENT)
        edge_lat = residual(edge_lat, mlp_tail(pre_act, w_edge_two))
        edge_sum = jnp.sum(edge_lat.reshape(MESH_NODES, OFFSET_COUNT, LATENT).astype(jnp.float32), axis=1).astype(jnp.bfloat16)
        mesh_cur = residual(mesh_cur, mlp_tail(matmul_f32(mesh_cur, w_node[:LATENT]) + matmul_f32(edge_sum, w_node[LATENT:]), w_node_two))
        return (mesh_cur, edge_lat), None

    def forecast_step(state_pair, force_now):
        state_prev, state_cur = state_pair
        features = jnp.concatenate([(state_prev - in_mean) / in_std, (state_cur - in_mean) / in_std, force_now, grid_static], axis=1)
        grid_lat = embed_static(features, w_grid_in, w_embed_out[0])
        w_first = w_edge_in[0]
        senders = jnp.roll(grid_lat, SHIFT * GRID_RATIO, axis=0)
        recv_term = matmul_f32(mesh_lat, w_first[2 * LATENT:])
        pre_act = matmul_f32(g2m_lat, w_first[:LATENT]) + matmul_f32(senders, w_first[LATENT:2 * LATENT])
        pre_act = (pre_act.reshape(MESH_NODES, GRID_RATIO, LATENT) + recv_term[:, None, :]).reshape(GRID_NODES, LATENT)
        enc_edge = residual(g2m_lat, mlp_tail(pre_act, w_edge_out[0]))
        enc_sum = jnp.sum(enc_edge.reshape(MESH_NODES, GRID_RATIO, LATENT).astype(jnp.float32), axis=1).astype(jnp.bfloat16)
        node_first = w_node_in[0]
        mesh_cur = residual(mesh_lat, mlp_tail(matmul_f32(mesh_lat, node_first[:LATENT]) + matmul_f32(enc_sum, node_first[LATENT:]), w_node_out[0]))
        grid_cur = residual(grid_lat, mlp_tail(matmul_f32(grid_lat, w_grid_self[0]), w_grid_self[1]))
        layer_weights = (w_edge_in[1:BLOCKS - 1], w_edge_out[1:BLOCKS - 1], w_node_in[1:BLOCKS - 1], w_node_out[1:BLOCKS - 1])
        layer_out, no_stack = lax.scan(proc_layer, (mesh_cur, edge_base), layer_weights)
        mesh_cur = layer_out[0]
        w_last = w_edge_in[BLOCKS - 1]
        send_term = matmul_f32(jnp.roll(mesh_cur, -SHIFT, axis=0), w_last[LATENT:2 * LATENT])
        pre_act = matmul_f32(m2g_lat, w_last[:LATENT]) + matmul_f32(grid_cur, w_last[2 * LATENT:])
        pre_act = (pre_act.reshape(MESH_NODES, GRID_RATIO, LATENT) + send_term[:, None, :]).reshape(GRID_NODES, LATENT)
        dec_edge = residual(m2g_lat, mlp_tail(pre_act, w_edge_out[BLOCKS - 1]))
        node_last = w_node_in[BLOCKS - 1]
        grid_out = residual(grid_cur, mlp_tail(matmul_f32(grid_cur, node_last[:LATENT]) + matmul_f32(dec_edge, node_last[LATENT:]), w_node_out[BLOCKS - 1]))
        hidden = jax.nn.silu(matmul_f32(grid_out, w_out_hidden)).astype(jnp.bfloat16)
        prediction = matmul_f32(hidden, w_out_final)
        state_next = state_cur + diff_std * prediction + diff_mean
        return (state_cur, state_next), state_next

    final_pair, stacked = lax.scan(forecast_step, (x_prev, x_cur), jnp.swapaxes(forcing, 0, 1))
    return stacked[0], stacked[1]
```

```python
import functools
import math

import jax
import jax.numpy as jnp
from jax import lax
from jax.experimental import pallas as pl
from jax.experimental.pallas import tpu as pltpu
from jax.sharding import PartitionSpec as P

F32 = jnp.float32
BF16 = jnp.bfloat16
LANES = 128
QUARTERS = 4
EDGE_KINDS = 6


def chip_ring(side):
    order = list(range(side))
    for y in range(1, side):
        columns = range(1, side)
        order += [y * side + x for x in (reversed(columns) if y % 2 else columns)]
    order += [y * side for y in range(side - 1, 0, -1)]
    return order


def dot(left, right):
    return jnp.dot(left, right, preferred_element_type=F32)


def silu(values):
    half = 0.5 * values
    return half + half * jnp.tanh(half)


def layer_norm(values):
    centred = values - jnp.mean(values, axis=-1, keepdims=True)
    spread = jnp.mean(centred * centred, axis=-1, keepdims=True)
    return centred * lax.rsqrt(spread + 1e-5)


def tail(pre_act, w_second):
    return layer_norm(dot(silu(pre_act).astype(BF16), w_second))


def pick(index, table):
    found = jnp.int32(0)
    for position, value in enumerate(table):
        found = found + jnp.where(index == position, jnp.int32(value), jnp.int32(0))
    return found


def rows_mod(shape, modulus):
    return lax.broadcasted_iota(jnp.int32, shape, 0) & (modulus - 1)


def next_quarter(values):
    rows = values.shape[0]
    return jnp.where(rows_mod(values.shape, 4) < 3, pltpu.roll(values, rows - 1, 0), pltpu.roll(values, 3, 0))


def prev_quarter(values):
    rows = values.shape[0]
    return jnp.where(rows_mod(values.shape, 4) > 0, pltpu.roll(values, 1, 0), pltpu.roll(values, rows - 3, 0))


def kernel(cfg, xp_in, xc_in, gf_in, mf_in, ns_in, wpad, wfin, wembed_h, win_h, wout_h, nin_h, nout_h, wself_h, whid_h,
           out_a, out_b,
           wembed, win, wout, nin, nout, wself, whid, state, perm, mf_next, mf_all, mf_blk,
           fst_s, fst_r, stage_s, stage_r, back_s, back_r,
           mesh_buf, edge_a, edge_b, halo_b, halo_c,
           edges, edge_base, mesh_lat, g2m_lat, m2g_lat, grid_lat, grid_cur,
           enc_base, enc_node, dec_base, dec_static, dec_node, mesh_band,
           proj, recv, node_pre, acc, tail_pre, beside, far,
           misc_sem, wl_sem, shift_sem, fst_ss, fst_rs, stg_ss, stg_rs, bck_ss, bck_rs, halo_ss, halo_rs):
    group, ring, latent, ratio, layers, half = cfg
    chips = len(ring)
    mesh_dev = chips * 8
    step_rows = mesh_dev // QUARTERS
    me = lax.axis_index("gp")
    core = me % 2
    where_of = [0] * chips
    for position, chip in enumerate(ring):
        where_of[chip] = position
    place = pick(me // 2, where_of)
    chip_up = pick(place, ring[1:] + ring[:1])
    chip_down = pick(place, ring[-1:] + ring[:-1])
    is_last = place == chips - 1
    is_first = place == 0
    band_core = (me % 8) // 4
    band_slot = (me // 8) * 4 + me % 4
    other = me + 1 - 2 * core

    def target(index):
        return dict(device_id={"gp": index}, device_id_type=pl.DeviceIdType.MESH)

    def local(source, dest, sem):
        return pltpu.make_async_copy(source, dest, sem)

    def block_copies(block, slot):
        return [local(win_h.at[block], win.at[slot], wl_sem.at[slot, 0]), local(wout_h.at[block], wout.at[slot], wl_sem.at[slot, 1]),
                local(nin_h.at[block], nin.at[slot], wl_sem.at[slot, 2]), local(nout_h.at[block], nout.at[slot], wl_sem.at[slot, 3])]

    embed_copy = local(wembed_h, wembed, misc_sem.at[0])
    self_copy = local(wself_h, wself, misc_sem.at[1])
    hid_copy = local(whid_h, whid, misc_sem.at[2])
    enc_copies = block_copies(0, 2)
    dec_copies = block_copies(layers + 1, 3)
    for copy in [embed_copy] + enc_copies + [self_copy] + dec_copies + [hid_copy] + block_copies(1, 0):
        copy.start()

    barrier = pltpu.get_barrier_semaphore()
    for hop in range(1, group):
        pl.semaphore_signal(barrier, inc=1, **target(lax.rem(me + hop, group)))

    row = lax.broadcasted_iota(jnp.int32, (mesh_dev, mesh_dev), 0)
    col = lax.broadcasted_iota(jnp.int32, (mesh_dev, mesh_dev), 1)

    def by_chip(index):
        return ((index >> 2) & 1) * half + (index >> 3) * 4 + (index & 3)

    def by_source(index):
        b = (index >> 2) & 7
        return ((index & 3) * 4 + (b >> 1)) * 8 + (b & 1) * 4 + (index >> 5)

    for slot, mask in enumerate((by_chip(row) == col, by_source(row) == col, row == by_source(col), row == by_chip(col))):
        perm[slot] = jnp.where(mask, 1.0, 0.0).astype(BF16)

    for ref in (halo_c, enc_base, enc_node, dec_base, dec_node, dec_static, acc, proj, recv, node_pre, tail_pre, beside, far):
        ref[...] = jnp.zeros_like(ref)
    state[...] = jnp.zeros_like(state)
    for r in range(ratio):
        state[0, r, :, :xp_in.shape[1]] = xp_in[pl.ds(r, mesh_dev, stride=ratio), :]
        state[1, r, :, :xc_in.shape[1]] = xc_in[pl.ds(r, mesh_dev, stride=ratio), :]

    pl.semaphore_wait(barrier, group - 1)
    shift = pltpu.make_async_remote_copy(mf_in.at[pl.ds(0, half)], mf_next, shift_sem.at[0], shift_sem.at[1],
                                         **target(lax.rem(me + group - 1, group)))
    shift.start()

    def exchange(src, dst, send_sem, recv_sem, slot, dest_of, source_of):
        copies = []
        for part in range(chips):
            dest = dest_of(part)
            copy = pltpu.make_async_remote_copy(src.at[part], dst.at[slot], send_sem.at[part], recv_sem.at[slot], **target(dest))
            copies.append((dest, copy))

            @pl.when(dest != me)
            def _(copy=copy):
                copy.start()

            @pl.when(dest == me)
            def _(part=part):
                dst[slot] = src[part]

        def finish():
            for part in range(chips):
                origin = source_of(part)

                @pl.when(origin != me)
                def _(part=part):
                    pltpu.make_async_remote_copy(src.at[part], dst.at[part], send_sem.at[part], recv_sem.at[part], **target(other)).wait_recv()

            for dest, copy in copies:
                @pl.when(dest != me)
                def _(copy=copy):
                    copy.wait_send()
        return finish

    def forth(src, dst, send_sem, recv_sem):
        return exchange(src, dst, send_sem, recv_sem, band_slot, lambda p: 2 * ring[p] + band_core,
                        lambda q: (q // 4) * 8 + core * 4 + q % 4)

    def back(src, dst, send_sem, recv_sem):
        return exchange(src, dst, send_sem, recv_sem, place, lambda q: (q // 4) * 8 + core * 4 + q % 4,
                        lambda p: 2 * ring[p] + band_core)

    embed_copy.wait()
    for r in range(ratio):
        m2g_lat[r] = tail(dot(gf_in[r], wpad[4]), wembed[3]).astype(BF16)
    shift.wait()
    mf_all[:half] = mf_in[half:]
    mf_all[half:] = mf_next[...]
    feats = mf_all[...]
    fst_s[...] = dot(perm[0], feats).astype(BF16).reshape(fst_s.shape)
    fst_done = forth(fst_s, fst_r, fst_ss, fst_rs)
    mesh_lat[...] = tail(dot(feats, wpad[5 + EDGE_KINDS]), wembed[1]).astype(BF16)
    for copy in enc_copies:
        copy.wait()
    recv[...] = dot(mesh_lat[...], win[2, 2 * latent:])
    enc_node[...] = dot(mesh_lat[...], nin[2, :latent])
    for r in range(ratio):
        g2m_lat[r] = tail(dot(feats, wpad[6 + EDGE_KINDS + r]), wembed[2]).astype(BF16)
        enc_base[r] = recv[...] + dot(g2m_lat[r], win[2, :latent])
    for copy in dec_copies:
        copy.wait()
    for r in range(ratio):
        dec_static[r] = dot(m2g_lat[r], win[3, :latent])
    fst_done()
    mf_blk[...] = dot(perm[1], fst_r[...].reshape(mesh_dev, LANES)).astype(BF16)
    for k in range(EDGE_KINDS):
        edge_base[k] = tail(dot(mf_blk[...], wpad[5 + k]), wembed[4]).astype(BF16)
    self_copy.wait()
    hid_copy.wait()

    low = lax.broadcasted_iota(jnp.int32, (8, latent), 0) < 4

    def put_mesh(slot, values):
        mesh_buf[slot] = values.astype(BF16)
        heads = [values[c * step_rows:c * step_rows + 8] for c in range(4)]
        tails = [values[(c + 1) * step_rows - 8:(c + 1) * step_rows] for c in range(4)]
        edge_a[slot] = jnp.concatenate([jnp.where(low, heads[0], pltpu.roll(heads[1], 4, 0)),
                                        jnp.where(low, heads[2], pltpu.roll(heads[3], 4, 0))], axis=0).astype(BF16)
        edge_b[slot] = jnp.concatenate([jnp.where(low, pltpu.roll(tails[0], 4, 0), tails[1]),
                                        jnp.where(low, pltpu.roll(tails[2], 4, 0), tails[3])], axis=0).astype(BF16)

    def halo_copies(slot):
        def send(src, dst, kind, dest):
            return pltpu.make_async_remote_copy(src, dst, halo_ss.at[slot, kind], halo_rs.at[slot, kind], **target(dest))
        near = [send(mesh_buf.at[slot, pl.ds(0, step_rows)], halo_c.at[slot, pl.ds(0, step_rows)], 0, 2 * chip_down + core),
                send(mesh_buf.at[slot, pl.ds(mesh_dev - step_rows, step_rows)], halo_c.at[slot, pl.ds(step_rows, step_rows)], 1, 2 * chip_up + core)]
        pair = [send(edge_a.at[slot], halo_b.at[slot, pl.ds(0, 16)], 2, other),
                send(edge_b.at[slot], halo_b.at[slot, pl.ds(16, 16)], 3, other)]
        seam_a = send(edge_a.at[slot], halo_c.at[slot, pl.ds(2 * step_rows, 16)], 4, 2 * chip_down + 1 - core)
        seam_b = send(edge_b.at[slot], halo_c.at[slot, pl.ds(2 * step_rows + 16, 16)], 5, 2 * chip_up + 1 - core)
        return near, pair, seam_a, seam_b

    def run_layer(step, layer):
        slot = layer % 2
        later = 1 - slot
        near, pair, seam_a, seam_b = halo_copies(slot)
        near[0].start()
        near[1].start()

        @pl.when(is_first)
        def _():
            seam_a.start()

        @pl.when(is_last)
        def _():
            seam_b.start()
        pair[0].start()
        pair[1].start()

        for copy in block_copies(layer + 1, slot):
            copy.wait()

        @pl.when(jnp.logical_or(step == 0, layer < layers - 1))
        def _():
            for copy in block_copies(1 + (layer + 1) % layers, later):
                copy.start()

        w_edge = win.at[slot]
        w_edge_two = wout.at[slot]
        w_node = nin.at[slot]
        w_node_two = nout.at[slot]

        @pl.when(layer == 0)
        def _():
            edges[...] = edge_base[...]

        nodes = mesh_buf[slot]
        proj[...] = dot(nodes, w_edge[latent:2 * latent])
        recv[...] = dot(nodes, w_edge[2 * latent:])

        def edge_part(kind, lo, hi, sent, first=False):
            old = edges[kind, lo:hi]
            pre = dot(old, w_edge[:latent]) + sent + recv[lo:hi]
            new = (old.astype(F32) + tail(pre, w_edge_two[...])).astype(BF16)
            edges[kind, lo:hi] = new
            if first:
                acc[lo:hi] = new.astype(F32)
            else:
                acc[lo:hi] = acc[lo:hi] + new.astype(F32)

        edge_part(4, 0, mesh_dev, next_quarter(proj[...]), first=True)
        edge_part(5, 0, mesh_dev, prev_quarter(proj[...]))
        edge_part(0, 0, mesh_dev - step_rows, proj[step_rows:])
        edge_part(1, step_rows, mesh_dev, proj[:mesh_dev - step_rows])
        node_pre[...] = dot(nodes, w_node[:latent])
        tail_pre[:step_rows] = dot(edges[0, mesh_dev - step_rows:], w_edge[:latent]) + recv[mesh_dev - step_rows:]
        tail_pre[step_rows:] = dot(edges[1, :step_rows], w_edge[:latent]) + recv[:step_rows]

        pair[0].wait_recv()
        pair[1].wait_recv()
        beside[...] = dot(halo_b[slot], w_edge[latent:2 * latent])
        above = jnp.where(core == 1, next_quarter(beside[:16]), beside[:16])
        below = jnp.where(core == 0, prev_quarter(beside[16:]), beside[16:])
        for kind, halo, shifted in ((2, above, pltpu.roll(proj[...], mesh_dev - 4, 0)), (3, below, pltpu.roll(proj[...], 4, 0))):
            parts = []
            for c in range(4):
                piece = halo[(c // 2) * 8:(c // 2) * 8 + 8]
                lo, hi = c * step_rows, (c + 1) * step_rows
                if kind == 2:
                    piece = piece if c % 2 else pltpu.roll(piece, 4, 0)
                    parts += [shifted[lo:hi - 8], jnp.where(low, shifted[hi - 8:hi], piece)]
                else:
                    piece = pltpu.roll(piece, 4, 0) if c % 2 else piece
                    parts += [jnp.where(low, piece, shifted[lo:lo + 8]), shifted[lo + 8:hi]]
            edge_part(kind, 0, mesh_dev, jnp.concatenate(parts, axis=0))

        near[0].wait_recv()
        near[1].wait_recv()

        @pl.when(is_last)
        def _():
            seam_a.wait_recv()

        @pl.when(is_first)
        def _():
            seam_b.wait_recv()
        far[...] = dot(halo_c[slot], w_edge[latent:2 * latent])
        up, down = far[:step_rows], far[step_rows:2 * step_rows]
        up_seam = far[2 * step_rows:2 * step_rows + 8]
        up_seam = pltpu.roll(jnp.where(core == 1, next_quarter(up_seam), up_seam), 4, 0)
        down_seam = far[2 * step_rows + 24:]
        down_seam = pltpu.roll(jnp.where(core == 0, prev_quarter(down_seam), down_seam), 4, 0)
        up_moved = pltpu.roll(up, step_rows - 4, 0)
        up_moved = jnp.concatenate([up_moved[:step_rows - 8], jnp.where(low, up_moved[step_rows - 8:], up_seam)], axis=0)
        down_moved = pltpu.roll(down, 4, 0)
        down_moved = jnp.concatenate([jnp.where(low, down_seam, down_moved[:8]), down_moved[8:]], axis=0)
        sent = jnp.concatenate([jnp.where(is_last, up_moved, up), jnp.where(is_first, down_moved, down)], axis=0)
        update = tail(tail_pre[...] + sent, w_edge_two[...])
        new_up = (edges[0, mesh_dev - step_rows:].astype(F32) + update[:step_rows]).astype(BF16)
        new_down = (edges[1, :step_rows].astype(F32) + update[step_rows:]).astype(BF16)
        edges[0, mesh_dev - step_rows:] = new_up
        edges[1, :step_rows] = new_down
        total = jnp.concatenate([acc[:step_rows] + new_down.astype(F32), acc[step_rows:mesh_dev - step_rows],
                                 acc[mesh_dev - step_rows:] + new_up.astype(F32)], axis=0).astype(BF16)
        update = tail(node_pre[...] + dot(total, w_node[latent:]), w_node_two[...])
        fresh = (nodes.astype(F32) + update).astype(BF16).astype(F32)
        near[0].wait_send()
        near[1].wait_send()
        pair[0].wait_send()
        pair[1].wait_send()

        @pl.when(is_first)
        def _():
            seam_a.wait_send()

        @pl.when(is_last)
        def _():
            seam_b.wait_send()
        put_mesh(later, fresh)

    mean, spread, diff_mean, diff_spread = ns_in[0:1], ns_in[1:2], ns_in[2:3], ns_in[3:4]

    def run_step(step):
        after = lax.rem(step + 2, 3)
        for r in range(ratio):
            past = ((state[step, r] - mean) / spread).astype(BF16)
            now = ((state[step + 1, r] - mean) / spread).astype(BF16)
            pre = dot(past, wpad[0]) + dot(now, wpad[1]) + dot(gf_in[r], wpad[2 + step])
            lat = tail(pre, wembed[0]).astype(BF16)
            grid_lat[r] = lat
            pre = enc_base[r] + dot(lat, win[2, latent:2 * latent])
            new = (g2m_lat[r].astype(F32) + tail(pre, wout[2])).astype(BF16).astype(F32)
            acc[...] = new if r == 0 else acc[...] + new
        update = tail(enc_node[...] + dot(acc[...].astype(BF16), nin[2, latent:]), nout[2])
        encoded = (mesh_lat[...].astype(F32) + update).astype(BF16)
        stage_s[...] = dot(perm[0], encoded).astype(BF16).reshape(stage_s.shape)
        arrive = forth(stage_s, stage_r, stg_ss, stg_rs)
        for r in range(ratio):
            lat = grid_lat[r]
            cur = (lat.astype(F32) + tail(dot(lat, wself[0]), wself[1])).astype(BF16)
            grid_cur[r] = cur
            dec_base[r] = dec_static[r] + dot(cur, win[3, 2 * latent:])
            dec_node[r] = dot(cur, nin[3, :latent])
        arrive()
        acc[...] = dot(perm[1], stage_r[...].reshape(mesh_dev, latent))
        put_mesh(0, acc[...])

        @pl.loop(0, layers)
        def _(layer):
            run_layer(step, layer)

        back_s[...] = dot(perm[2], mesh_buf[layers % 2]).astype(BF16).reshape(back_s.shape)
        back(back_s, back_r, bck_ss, bck_rs)()
        mesh_band[...] = dot(perm[3], back_r[...].reshape(mesh_dev, latent)).astype(BF16)
        recv[...] = dot(mesh_band[...], win[3, latent:2 * latent])
        for r in range(ratio):
            dec_edge = (m2g_lat[r].astype(F32) + tail(dec_base[r] + recv[...], wout[3])).astype(BF16)
            update = tail(dec_node[r] + dot(dec_edge, nin[3, latent:]), nout[3])
            grid_out = (grid_cur[r].astype(F32) + update).astype(BF16)
            hidden = silu(dot(grid_out, whid[...])).astype(BF16)
            fresh = state[step + 1, r] + diff_spread * dot(hidden, wfin[...]) + diff_mean
            state[after, r] = fresh

            @pl.when(step == 0)
            def _():
                out_a[pl.ds(r, mesh_dev, stride=ratio), :] = fresh[:, :out_a.shape[1]]

            @pl.when(step == 1)
            def _():
                out_b[pl.ds(r, mesh_dev, stride=ratio), :] = fresh[:, :out_b.shape[1]]

    @pl.loop(0, 2)
    def _(step):
        run_step(step)


def solution(mesh):
    group = mesh.shape["gp"]
    side = math.isqrt(group // 2)
    ring = chip_ring(side)
    row_spec = P(("dp", "gp"))
    edge_spec = P(("dp", "gp"), None, None)
    whole = P()

    def local_run(x_prev, x_cur, forcing, grid_static, g2m_feat, m2g_feat, mesh_feat, mesh_edge_feat, norm_stats, w_grid_in, w_mesh_in, w_eemb_in, w_embed_out, w_edge_in, w_edge_out, w_node_in, w_node_out, w_grid_self, w_out_hidden, w_out_final):
        grid_dev, variables = x_prev.shape
        mesh_dev = mesh_feat.shape[0]
        ratio = grid_dev // mesh_dev
        latent = w_embed_out.shape[-1]
        layers = w_edge_in.shape[0] - 2
        steps, force = forcing.shape[1:]
        fixed = grid_static.shape[1]
        efeat = m2g_feat.shape[1]
        assert side * side * 2 == group and mesh_dev == 8 * len(ring) and mesh_dev == 128 and ratio == 4 and layers % 2 == 0

        def lanes(values, fill=0):
            return jnp.pad(values, [(0, 0)] * (values.ndim - 1) + [(0, LANES - values.shape[-1])], constant_values=fill)

        gf = jnp.concatenate([forcing.reshape(grid_dev, steps * force), grid_static, m2g_feat], axis=1).astype(BF16)
        gf = lanes(gf.reshape(mesh_dev, ratio, gf.shape[1]).transpose(1, 0, 2))
        kinds = mesh_edge_feat.shape[1]
        mf = lanes(jnp.concatenate([mesh_edge_feat.reshape(mesh_dev, kinds * efeat), mesh_feat,
                                    g2m_feat.reshape(mesh_dev, ratio * efeat)], axis=1).astype(BF16))
        ns = jnp.stack([lanes(norm_stats[0]), lanes(norm_stats[1], 1), lanes(norm_stats[2]), lanes(norm_stats[3])])

        def placed(*pieces):
            total = 0
            for start, rows in pieces:
                total = total + jnp.pad(rows, ((start, LANES - start - rows.shape[0]), (0, 0)))
            return total

        w_force = w_grid_in[2 * variables:2 * variables + force]
        w_fixed = w_grid_in[2 * variables + force:]
        start = steps * force
        pads = [placed((0, w_grid_in[:variables])), placed((0, w_grid_in[variables:2 * variables])),
                placed((0, w_force), (start, w_fixed)), placed((force, w_force), (start, w_fixed)),
                placed((start + fixed, w_eemb_in[1]))]
        pads += [placed((k * efeat, w_eemb_in[2])) for k in range(kinds)]
        pads += [placed((kinds * efeat, w_mesh_in))]
        pads += [placed((kinds * efeat + mesh_feat.shape[1] + r * efeat, w_eemb_in[0])) for r in range(ratio)]
        wpad = jnp.stack(pads)
        wfin = lanes(w_out_final)

        vmem = pl.BlockSpec(memory_space=pltpu.VMEM)
        hbm = pl.BlockSpec(memory_space=pl.ANY)
        chips = len(ring)
        step_rows = mesh_dev // QUARTERS
        VM = pltpu.VMEM
        DMA = pltpu.SemaphoreType.DMA
        grid_shape = (ratio, mesh_dev, latent)
        scratch = [
            VM(w_embed_out.shape, BF16), VM((4,) + w_edge_in.shape[1:], BF16), VM((4,) + w_edge_out.shape[1:], BF16),
            VM((4,) + w_node_in.shape[1:], BF16), VM((4,) + w_node_out.shape[1:], BF16), VM(w_grid_self.shape, BF16), VM(w_out_hidden.shape, BF16),
            VM((3, ratio, mesh_dev, LANES), F32), VM((4, mesh_dev, mesh_dev), BF16),
            VM((mesh_dev // 2, LANES), BF16), VM((mesh_dev, LANES), BF16), VM((mesh_dev, LANES), BF16),
            VM((chips, 8, LANES), BF16), VM((chips, 8, LANES), BF16),
            VM((chips, 8, latent), BF16), VM((chips, 8, latent), BF16), VM((chips, 8, latent), BF16), VM((chips, 8, latent), BF16),
            VM((2, mesh_dev, latent), BF16), VM((2, 16, latent), BF16), VM((2, 16, latent), BF16), VM((2, 32, latent), BF16), VM((2, 2 * step_rows + 32, latent), BF16),
            VM((EDGE_KINDS, mesh_dev, latent), BF16), VM((EDGE_KINDS, mesh_dev, latent), BF16), VM((mesh_dev, latent), BF16),
            VM(grid_shape, BF16), VM(grid_shape, BF16), VM(grid_shape, BF16), VM(grid_shape, BF16),
            VM(grid_shape, F32), VM((mesh_dev, latent), F32), VM(grid_shape, F32), VM(grid_shape, F32), VM(grid_shape, F32), VM((mesh_dev, latent), BF16),
            VM((mesh_dev, latent), F32), VM((mesh_dev, latent), F32), VM((mesh_dev, latent), F32), VM((mesh_dev, latent), F32), VM((2 * step_rows, latent), F32), VM((32, latent), F32), VM((2 * step_rows + 32, latent), F32),
            DMA((3,)), DMA((4, 4)), DMA((2,)), DMA((chips,)), DMA((chips,)), DMA((chips,)), DMA((chips,)), DMA((chips,)), DMA((chips,)), DMA((2, 6)), DMA((2, 6)),
        ]
        cfg = (group, ring, latent, ratio, layers, mesh_dev // 2)
        return pl.pallas_call(
            functools.partial(kernel, cfg),
            out_shape=(jax.ShapeDtypeStruct(x_cur.shape, F32),) * 2,
            in_specs=[vmem] * 7 + [hbm] * 7,
            out_specs=(vmem, vmem),
            scratch_shapes=scratch,
            compiler_params=pltpu.CompilerParams(collective_id=0, has_side_effects=True, vmem_limit_bytes=60 * 1024 * 1024),
        )(x_prev, x_cur, gf, mf, ns, wpad, wfin, w_embed_out, w_edge_in, w_edge_out, w_node_in, w_node_out, w_grid_self, w_out_hidden)

    in_specs = (row_spec, row_spec, edge_spec, row_spec, row_spec, row_spec, row_spec, edge_spec, whole) + (whole,) * 11
    return jax.shard_map(local_run, mesh=mesh, in_specs=in_specs, out_specs=(row_spec, row_spec), check_vma=False)
```

```python
import functools
import math

import jax
import jax.numpy as jnp
from jax import lax
from jax.experimental import pallas as pl
from jax.experimental.pallas import tpu as pltpu
from jax.sharding import PartitionSpec as P

F32 = jnp.float32
BF16 = jnp.bfloat16
LANES = 128
EDGE_KINDS = 6


def chip_ring(side):
    order = list(range(side))
    for y in range(1, side):
        columns = range(1, side)
        order += [y * side + x for x in (reversed(columns) if y % 2 else columns)]
    order += [y * side for y in range(side - 1, 0, -1)]
    return order


def dot(left, right):
    return jnp.dot(left, right, preferred_element_type=F32)


def silu(values):
    half = 0.5 * values
    return half + half * jnp.tanh(half)


def layer_norm(values):
    centred = values - jnp.mean(values, axis=-1, keepdims=True)
    spread = jnp.mean(centred * centred, axis=-1, keepdims=True)
    return centred * lax.rsqrt(spread + 1e-5)


def tail(pre_act, w_second):
    return layer_norm(dot(silu(pre_act).astype(BF16), w_second))


def pick(index, table):
    found = jnp.int32(0)
    for position, value in enumerate(table):
        found = found + jnp.where(index == position, jnp.int32(value), jnp.int32(0))
    return found


def rows_mod(shape, modulus):
    return lax.broadcasted_iota(jnp.int32, shape, 0) & (modulus - 1)


def next_quarter(values):
    rows = values.shape[0]
    return jnp.where(rows_mod(values.shape, 4) < 3, pltpu.roll(values, rows - 1, 0), pltpu.roll(values, 3, 0))


def prev_quarter(values):
    rows = values.shape[0]
    return jnp.where(rows_mod(values.shape, 4) > 0, pltpu.roll(values, 1, 0), pltpu.roll(values, rows - 3, 0))


def kernel(cfg, xp_h, xc_h, frc_in, fix_in, m2g_in, g2m_in, mef_in, mft_in, ns_in, wpad, wfin, wembed_h, win_h, wout_h, nin_h, nout_h, wself_h, whid_h,
           out_a, out_b,
           xbuf, tbuf, nat, mt, gf_in, mf_in, wembed, win, wout, nin, nout, wself, whid, state, perm, mf_next, mf_all, mf_blk,
           fst_s, fst_r, stage_s, stage_r, back_s, back_r, mesh_buf, halo,
           edges, edge_base, mesh_lat, g2m_lat, m2g_lat, grid_lat, grid_cur,
           enc_base, enc_node, dec_base, dec_static, dec_node, mesh_band,
           proj, recv, node_pre, acc, pre_ref, far,
           misc_sem, wl_sem, shift_sem, fst_ss, fst_rs, stg_ss, stg_rs, bck_ss, bck_rs, halo_ss, halo_rs):
    group, ring, latent, ratio, layers, half = cfg
    chips = len(ring)
    mesh_dev = 2 * half
    grid_dev = ratio * mesh_dev
    chunk = grid_dev // 2
    devices = [2 * ring[q // 2] + q % 2 for q in range(group)]
    me = lax.axis_index("gp")
    core = me % 2
    where_of = [0] * chips
    for position, chip in enumerate(ring):
        where_of[chip] = position
    chip_place = pick(me // 2, where_of)
    place = 2 * chip_place + core
    up = jnp.where(core == 0, me + 1, 2 * pick(chip_place, ring[1:] + ring[:1]))
    down = jnp.where(core == 1, me - 1, 2 * pick(chip_place, ring[-1:] + ring[:-1]) + 1)

    def target(index):
        return dict(device_id={"gp": index}, device_id_type=pl.DeviceIdType.MESH)

    def local(source, dest, sem):
        return pltpu.make_async_copy(source, dest, sem)

    def block_copies(block, slot):
        return [local(win_h.at[block], win.at[slot], wl_sem.at[slot, 0]), local(wout_h.at[block], wout.at[slot], wl_sem.at[slot, 1]),
                local(nin_h.at[block], nin.at[slot], wl_sem.at[slot, 2]), local(nout_h.at[block], nout.at[slot], wl_sem.at[slot, 3])]

    x_copies = [local(xp_h, xbuf.at[0], misc_sem.at[3]), local(xc_h, xbuf.at[1], misc_sem.at[4])]
    embed_copy = local(wembed_h, wembed, misc_sem.at[0])
    self_copy = local(wself_h, wself, misc_sem.at[1])
    hid_copy = local(whid_h, whid, misc_sem.at[2])
    enc_copies = block_copies(0, 2)
    dec_copies = block_copies(layers + 1, 3)
    for copy in [embed_copy] + x_copies + enc_copies + [self_copy] + dec_copies + [hid_copy] + block_copies(1, 0):
        copy.start()

    barrier = pltpu.get_barrier_semaphore()
    for hop in range(1, group):
        pl.semaphore_signal(barrier, inc=1, **target(lax.rem(me + hop, group)))

    row = lax.broadcasted_iota(jnp.int32, (mesh_dev, mesh_dev), 0)
    col = lax.broadcasted_iota(jnp.int32, (mesh_dev, mesh_dev), 1)

    def by_target(index):
        return ((index >> 1) & 1) * half + (index >> 2) * 2 + (index & 1)

    def by_source(index):
        b = (index >> 2) & 15
        return ((index & 3) * 8 + (b >> 1)) * 4 + (b & 1) * 2 + (index >> 6)

    for slot, mask in enumerate((by_target(row) == col, by_source(row) == col, row == by_source(col), row == by_target(col))):
        perm[slot] = jnp.where(mask, 1.0, 0.0).astype(BF16)

    for ref in (enc_base, enc_node, dec_base, dec_node, dec_static, acc, proj, recv, node_pre, pre_ref, far, state, tbuf, mt):
        ref[...] = jnp.zeros_like(ref)
    def halves():
        return [(part * chunk, (part + 1) * chunk) for part in range(2)]

    steps, force = frc_in.shape[1], frc_in.shape[0]
    fixed, efeat = fix_in.shape[0], m2g_in.shape[0]
    for f in range(force):
        for which in range(steps):
            tbuf[which * force + f:which * force + f + 1] = frc_in[f, which:which + 1]
    at = steps * force
    tbuf[at:at + fixed] = fix_in[...]
    at += fixed
    tbuf[at:at + efeat] = m2g_in[...]
    at += efeat
    tbuf[at:at + efeat] = g2m_in[...]
    nat[...] = tbuf[...].T
    for k in range(EDGE_KINDS):
        mt[k * efeat:(k + 1) * efeat] = mef_in[k]
    base = EDGE_KINDS * efeat
    mt[base:base + mft_in.shape[0]] = mft_in[...]
    base += mft_in.shape[0]
    turned = mt[...].T
    lane = lax.broadcasted_iota(jnp.int32, turned.shape, 1)
    for r in range(ratio):
        rows = nat[pl.ds(r, mesh_dev, stride=ratio), :]
        gf_in[r * mesh_dev:(r + 1) * mesh_dev] = rows.astype(BF16)
        first = base + r * efeat
        turned = jnp.where(jnp.logical_and(lane >= first, lane < first + efeat), pltpu.roll(rows, first - at, 1), turned)
    mf_in[...] = turned.astype(BF16)
    tbuf[...] = jnp.zeros_like(tbuf)
    embed_copy.wait()
    for lo, hi in halves()[:1]:
        m2g_lat[lo:hi] = tail(dot(gf_in[lo:hi], wpad[4]), wembed[3]).astype(BF16)
    pl.semaphore_wait(barrier, group - 1)
    shift = pltpu.make_async_remote_copy(mf_in.at[pl.ds(0, half)], mf_next, shift_sem.at[0], shift_sem.at[1],
                                         **target(lax.rem(me + group - 1, group)))
    shift.start()

    def exchange(src, dst, send_sem, recv_sem, slot, dest_of, source_of):
        copies = []
        for part in range(group):
            dest = dest_of(part)
            copy = pltpu.make_async_remote_copy(src.at[part], dst.at[slot], send_sem.at[part], recv_sem.at[slot], **target(dest))
            copies.append((dest, copy))

            @pl.when(dest != me)
            def _(copy=copy):
                copy.start()

            @pl.when(dest == me)
            def _(part=part):
                dst[slot] = src[part]

        def finish():
            for part in range(group):
                @pl.when(source_of(part) != me)
                def _(part=part):
                    pltpu.make_async_remote_copy(src.at[part], dst.at[part], send_sem.at[part], recv_sem.at[part], **target(up)).wait_recv()

            for dest, copy in copies:
                @pl.when(dest != me)
                def _(copy=copy):
                    copy.wait_send()
        return finish

    def forth(src, dst, send_sem, recv_sem):
        return exchange(src, dst, send_sem, recv_sem, me, lambda q: devices[q], lambda d: d)

    def back(src, dst, send_sem, recv_sem):
        return exchange(src, dst, send_sem, recv_sem, place, lambda d: d, lambda q: devices[q])

    for lo, hi in halves()[1:]:
        m2g_lat[lo:hi] = tail(dot(gf_in[lo:hi], wpad[4]), wembed[3]).astype(BF16)
    for copy in x_copies:
        copy.wait()
    for which in range(2):
        tbuf[:xbuf.shape[1]] = xbuf[which]
        nat[...] = tbuf[...].T
        for r in range(ratio):
            state[which, r * mesh_dev:(r + 1) * mesh_dev] = nat[pl.ds(r, mesh_dev, stride=ratio), :]
    shift.wait()
    mf_all[:half] = mf_in[half:]
    mf_all[half:] = mf_next[...]
    feats = mf_all[...]
    fst_s[...] = dot(perm[0], feats).astype(BF16).reshape(fst_s.shape)
    fst_done = forth(fst_s, fst_r, fst_ss, fst_rs)
    mesh_lat[...] = tail(dot(feats, wpad[5 + EDGE_KINDS]), wembed[1]).astype(BF16)
    for copy in enc_copies:
        copy.wait()
    recv[...] = dot(mesh_lat[...], win[2, 2 * latent:])
    enc_node[...] = dot(mesh_lat[...], nin[2, :latent])
    for r in range(ratio):
        dec_base[r * mesh_dev:(r + 1) * mesh_dev] = dot(feats, wpad[6 + EDGE_KINDS + r])
    for lo, hi in halves():
        g2m_lat[lo:hi] = tail(dec_base[lo:hi], wembed[2]).astype(BF16)
    for lo, hi in halves():
        dec_node[lo:hi] = dot(g2m_lat[lo:hi], win[2, :latent])
    for r in range(ratio):
        rows = slice(r * mesh_dev, (r + 1) * mesh_dev)
        enc_base[rows] = dec_node[rows] + recv[...]
    for copy in dec_copies:
        copy.wait()
    for lo, hi in halves():
        dec_static[lo:hi] = dot(m2g_lat[lo:hi], win[3, :latent])
    self_copy.wait()
    hid_copy.wait()

    top, low_end = 4 * mesh_dev, 5 * mesh_dev
    near_index, far_index = core, 1 - core
    side_row = lax.broadcasted_iota(jnp.int32, (half, latent), 0)

    def step_up(values):
        moved = pltpu.roll(values, half - 4, 0)
        return jnp.where(side_row >= half - 4, next_quarter(moved), moved)

    def step_down(values):
        moved = pltpu.roll(values, 4, 0)
        return jnp.where(side_row < 4, prev_quarter(moved), moved)

    def run_layer(step, layer):
        slot = layer % 2
        later = 1 - slot

        def send(part, dest):
            return pltpu.make_async_remote_copy(mesh_buf.at[slot, pl.ds(part * half, half)], halo.at[slot, part],
                                                halo_ss.at[slot, part], halo_rs.at[slot, part], **target(dest))
        to_down, to_up = send(0, down), send(1, up)

        @pl.when(core == 0)
        def _():
            to_down.start()
            to_up.start()

        @pl.when(core == 1)
        def _():
            to_up.start()
            to_down.start()

        for copy in block_copies(layer + 1, slot):
            copy.wait()

        @pl.when(jnp.logical_or(step == 0, layer < layers - 1))
        def _():
            for copy in block_copies(1 + (layer + 1) % layers, later):
                copy.start()

        @pl.when(layer == 0)
        def _():
            edges[...] = edge_base[...]

        w_edge = win.at[slot]
        w_edge_two = wout.at[slot]
        w_node = nin.at[slot]
        w_node_two = nout.at[slot]
        nodes = mesh_buf[slot]
        proj[...] = dot(nodes, w_edge[latent:2 * latent])
        recv[...] = dot(nodes, w_edge[2 * latent:])
        pre_ref[...] = dot(edges[...], w_edge[:latent])

        def renew(lo, rows, sent):
            hidden = silu(pre_ref[lo:lo + sent.shape[0]] + sent + rows).astype(BF16)
            return hidden

        everyone = recv[...]
        hidden_a = jnp.concatenate([
            renew(2 * mesh_dev, everyone, next_quarter(proj[...])),
            renew(3 * mesh_dev, everyone, prev_quarter(proj[...])),
            renew(top, everyone, jnp.concatenate([proj[half:], proj[:half]], axis=0))], axis=0)
        out_a_rows = dot(hidden_a, w_edge_two[...])
        hidden_b = jnp.concatenate([
            renew(0, everyone, jnp.concatenate([step_up(proj[:half]), step_up(proj[half:])], axis=0)),
            renew(mesh_dev, everyone, jnp.concatenate([step_down(proj[:half]), step_down(proj[half:])], axis=0))], axis=0)
        out_b_rows = dot(hidden_b, w_edge_two[...])
        node_pre[...] = dot(nodes, w_node[:latent])

        def settle(lo, values, first=False):
            new = (edges[lo:lo + mesh_dev].astype(F32) + layer_norm(values)).astype(BF16)
            edges[lo:lo + mesh_dev] = new
            acc[...] = new.astype(F32) if first else acc[...] + new.astype(F32)

        settle(2 * mesh_dev, out_a_rows[:mesh_dev], first=True)
        settle(3 * mesh_dev, out_a_rows[mesh_dev:2 * mesh_dev])
        settle(top, out_a_rows[2 * mesh_dev:])
        settle(0, out_b_rows[:mesh_dev])
        settle(mesh_dev, out_b_rows[mesh_dev:])

        def side(index, sent):
            lo = pl.multiple_of(low_end + index * half, half)
            into = pl.multiple_of((1 - index) * half, half)
            pre = pre_ref[pl.ds(lo, half)] + sent + recv[pl.ds(into, half)]
            new = (edges[pl.ds(lo, half)].astype(F32) + tail(pre, w_edge_two[...])).astype(BF16)
            edges[pl.ds(lo, half)] = new
            acc[pl.ds(into, half)] = acc[pl.ds(into, half)] + new.astype(F32)

        def arrived(index):
            pltpu.make_async_remote_copy(mesh_buf.at[slot, pl.ds(0, half)], halo.at[slot, index],
                                         halo_ss.at[slot, index], halo_rs.at[slot, index], **target(up)).wait_recv()

        arrived(near_index)
        far[...] = dot(halo[slot, near_index], w_edge[latent:2 * latent])
        side(near_index, far[...])
        arrived(far_index)
        far[...] = dot(halo[slot, far_index], w_edge[latent:2 * latent])
        sent = far[...]
        sent = jnp.where(place == group - 1, step_up(sent), jnp.where(place == 0, step_down(sent), sent))
        side(far_index, sent)
        update = tail(node_pre[...] + dot(acc[...].astype(BF16), w_node[latent:]), w_node_two[...])
        to_down.wait_send()
        to_up.wait_send()
        mesh_buf[later] = (nodes.astype(F32) + update).astype(BF16)

    mean, spread, diff_mean, diff_spread = ns_in[0:1], ns_in[1:2], ns_in[2:3], ns_in[3:4]

    def run_step(step):
        after = lax.rem(step + 2, 3)
        for lo, hi in halves():
            past = ((state[step, lo:hi] - mean) / spread).astype(BF16)
            now = ((state[step + 1, lo:hi] - mean) / spread).astype(BF16)
            pre = dot(past, wpad[0]) + dot(now, wpad[1]) + dot(gf_in[lo:hi], wpad[2 + step])
            grid_lat[lo:hi] = tail(pre, wembed[0]).astype(BF16)
        for part, (lo, hi) in enumerate(halves()):
            pre = enc_base[lo:hi] + dot(grid_lat[lo:hi], win[2, latent:2 * latent])
            new = (g2m_lat[lo:hi].astype(F32) + tail(pre, wout[2])).astype(BF16).astype(F32)
            total = new[:mesh_dev] + new[mesh_dev:]
            acc[...] = total if part == 0 else acc[...] + total
        update = tail(enc_node[...] + dot(acc[...].astype(BF16), nin[2, latent:]), nout[2])
        mesh_band[...] = (mesh_lat[...].astype(F32) + update).astype(BF16)
        stage_s[...] = dot(perm[0], mesh_band[...]).astype(BF16).reshape(stage_s.shape)
        arrive = forth(stage_s, stage_r, stg_ss, stg_rs)
        for lo, hi in halves():
            lat = grid_lat[lo:hi]
            grid_cur[lo:hi] = (lat.astype(F32) + tail(dot(lat, wself[0]), wself[1])).astype(BF16)

        @pl.when(step == 0)
        def _():
            fst_done()
            mf_blk[...] = dot(perm[1], fst_r[...].reshape(mesh_dev, LANES)).astype(BF16)
            for k in range(2, EDGE_KINDS):
                pre_ref[(k - 2) * mesh_dev:(k - 1) * mesh_dev] = dot(mf_blk[...], wpad[5 + k])
            pre_ref[top:top + half] = dot(mf_blk[:half], wpad[5])
            pre_ref[top + half:low_end] = dot(mf_blk[half:], wpad[6])
            pre_ref[low_end:low_end + half] = dot(mf_blk[half:], wpad[5])
            pre_ref[low_end + half:] = dot(mf_blk[:half], wpad[6])
            for lo in range(0, EDGE_KINDS * mesh_dev, chunk):
                edge_base[lo:lo + chunk] = tail(pre_ref[lo:lo + chunk], wembed[4]).astype(BF16)

        arrive()
        mesh_buf[0] = dot(perm[1], stage_r[...].reshape(mesh_dev, latent)).astype(BF16)

        @pl.loop(0, layers)
        def _(layer):
            run_layer(step, layer)

        back_s[...] = dot(perm[2], mesh_buf[layers % 2]).astype(BF16).reshape(back_s.shape)
        arrive = back(back_s, back_r, bck_ss, bck_rs)
        for lo, hi in halves():
            dec_base[lo:hi] = dec_static[lo:hi] + dot(grid_cur[lo:hi], win[3, 2 * latent:])
            dec_node[lo:hi] = dot(grid_cur[lo:hi], nin[3, :latent])
        arrive()
        mesh_band[...] = dot(perm[3], back_r[...].reshape(mesh_dev, latent)).astype(BF16)
        recv[...] = dot(mesh_band[...], win[3, latent:2 * latent])
        for lo, hi in halves():
            pre = dec_base[lo:hi] + jnp.concatenate([recv[...], recv[...]], axis=0)
            dec_edge = (m2g_lat[lo:hi].astype(F32) + tail(pre, wout[3])).astype(BF16)
            update = tail(dec_node[lo:hi] + dot(dec_edge, nin[3, latent:]), nout[3])
            grid_out = (grid_cur[lo:hi].astype(F32) + update).astype(BF16)
            hidden = silu(dot(grid_out, whid[...])).astype(BF16)
            state[after, lo:hi] = state[step + 1, lo:hi] + diff_spread * lax.dot_general(hidden, wfin[...], (((1,), (1,)), ((), ())), preferred_element_type=F32) + diff_mean
        for r in range(ratio):
            nat[pl.ds(r, mesh_dev, stride=ratio), :] = state[after, r * mesh_dev:(r + 1) * mesh_dev]
        tbuf[...] = nat[...].T

        @pl.when(step == 0)
        def _():
            out_a[...] = tbuf[:out_a.shape[0]]

        @pl.when(step == 1)
        def _():
            out_b[...] = tbuf[:out_b.shape[0]]

    @pl.loop(0, 2)
    def _(step):
        run_step(step)


def solution(mesh):
    group = mesh.shape["gp"]
    side = math.isqrt(group // 2)
    ring = chip_ring(side)
    row_spec = P(("dp", "gp"))
    edge_spec = P(("dp", "gp"), None, None)
    whole = P()

    def local_run(x_prev, x_cur, forcing, grid_static, g2m_feat, m2g_feat, mesh_feat, mesh_edge_feat, norm_stats, w_grid_in, w_mesh_in, w_eemb_in, w_embed_out, w_edge_in, w_edge_out, w_node_in, w_node_out, w_grid_self, w_out_hidden, w_out_final):
        grid_dev, variables = x_prev.shape
        mesh_dev = mesh_feat.shape[0]
        ratio = grid_dev // mesh_dev
        latent = w_embed_out.shape[-1]
        layers = w_edge_in.shape[0] - 2
        steps, force = forcing.shape[1:]
        fixed = grid_static.shape[1]
        efeat = m2g_feat.shape[1]
        assert side * side * 2 == group and mesh_dev == 8 * len(ring) and mesh_dev == 128 and ratio == 4 and layers % 2 == 0

        def lanes(values, fill=0):
            return jnp.pad(values, [(0, 0)] * (values.ndim - 1) + [(0, LANES - values.shape[-1])], constant_values=fill)

        kinds = mesh_edge_feat.shape[1]
        ns = jnp.stack([lanes(norm_stats[0]), lanes(norm_stats[1], 1), lanes(norm_stats[2]), lanes(norm_stats[3])])

        def placed(*pieces):
            total = 0
            for start, rows in pieces:
                total = total + jnp.pad(rows, ((start, LANES - start - rows.shape[0]), (0, 0)))
            return total

        w_force = w_grid_in[2 * variables:2 * variables + force]
        w_fixed = w_grid_in[2 * variables + force:]
        start = steps * force
        pads = [placed((0, w_grid_in[:variables])), placed((0, w_grid_in[variables:2 * variables])),
                placed((0, w_force), (start, w_fixed)), placed((force, w_force), (start, w_fixed)),
                placed((start + fixed, w_eemb_in[1]))]
        pads += [placed((k * efeat, w_eemb_in[2])) for k in range(kinds)]
        pads += [placed((kinds * efeat, w_mesh_in))]
        pads += [placed((kinds * efeat + mesh_feat.shape[1] + r * efeat, w_eemb_in[0])) for r in range(ratio)]
        wpad = jnp.stack(pads)
        wfin = jnp.pad(w_out_final.T, ((0, LANES - variables), (0, 0)))

        vmem = pl.BlockSpec(memory_space=pltpu.VMEM)
        hbm = pl.BlockSpec(memory_space=pl.ANY)
        VM = pltpu.VMEM
        DMA = pltpu.SemaphoreType.DMA
        grid_shape = (grid_dev, latent)
        node_shape = (mesh_dev, latent)
        part_shape = (group, mesh_dev // group, latent)
        feat_shape = part_shape[:2] + (LANES,)
        edge_shape = (EDGE_KINDS * mesh_dev, latent)
        half = mesh_dev // 2
        scratch = [
            VM((2, variables, grid_dev), F32), VM((LANES, grid_dev), F32), VM((grid_dev, LANES), F32), VM((LANES, mesh_dev), F32), VM((grid_dev, LANES), BF16), VM((mesh_dev, LANES), BF16),
            VM(w_embed_out.shape, BF16), VM((4,) + w_edge_in.shape[1:], BF16), VM((4,) + w_edge_out.shape[1:], BF16),
            VM((4,) + w_node_in.shape[1:], BF16), VM((4,) + w_node_out.shape[1:], BF16), VM(w_grid_self.shape, BF16), VM(w_out_hidden.shape, BF16),
            VM((3, grid_dev, LANES), F32), VM((4, mesh_dev, mesh_dev), BF16),
            VM((half, LANES), BF16), VM((mesh_dev, LANES), BF16), VM((mesh_dev, LANES), BF16),
            VM(feat_shape, BF16), VM(feat_shape, BF16), VM(part_shape, BF16), VM(part_shape, BF16), VM(part_shape, BF16), VM(part_shape, BF16),
            VM((2,) + node_shape, BF16), VM((2, 2, half, latent), BF16),
            VM(edge_shape, BF16), VM(edge_shape, BF16), VM(node_shape, BF16),
            VM(grid_shape, BF16), VM(grid_shape, BF16), VM(grid_shape, BF16), VM(grid_shape, BF16),
            VM(grid_shape, F32), VM(node_shape, F32), VM(grid_shape, F32), VM(grid_shape, F32), VM(grid_shape, F32), VM(node_shape, BF16),
            VM(node_shape, F32), VM(node_shape, F32), VM(node_shape, F32), VM(node_shape, F32), VM(edge_shape, F32), VM((half, latent), F32),
            DMA((5,)), DMA((4, 4)), DMA((2,)), DMA((group,)), DMA((group,)), DMA((group,)), DMA((group,)), DMA((group,)), DMA((group,)), DMA((2, 2)), DMA((2, 2)),
        ]
        cfg = (group, ring, latent, ratio, layers, mesh_dev // 2)
        next_t, after_t = pl.pallas_call(
            functools.partial(kernel, cfg),
            out_shape=(jax.ShapeDtypeStruct((variables, grid_dev), F32),) * 2,
            in_specs=[hbm] * 2 + [vmem] * 9 + [hbm] * 7,
            out_specs=(vmem, vmem),
            scratch_shapes=scratch,
            compiler_params=pltpu.CompilerParams(collective_id=0, has_side_effects=True, vmem_limit_bytes=60 * 1024 * 1024),
        )(x_prev.T, x_cur.T, forcing.transpose(2, 1, 0), grid_static.T, m2g_feat.T, g2m_feat.T, mesh_edge_feat.transpose(1, 2, 0), mesh_feat.T, ns, wpad, wfin,
          w_embed_out, w_edge_in, w_edge_out, w_node_in, w_node_out, w_grid_self, w_out_hidden)
        return next_t.T, after_t.T

    in_specs = (row_spec, row_spec, edge_spec, row_spec, row_spec, row_spec, row_spec, edge_spec, whole) + (whole,) * 11
    return jax.shard_map(local_run, mesh=mesh, in_specs=in_specs, out_specs=(row_spec, row_spec), check_vma=False)
```

```python
import functools
import math

import jax
import jax.numpy as jnp
from jax import lax
from jax.experimental import pallas as pl
from jax.experimental.pallas import tpu as pltpu
from jax.sharding import PartitionSpec as P

F32 = jnp.float32
BF16 = jnp.bfloat16
LANES = 128
EDGE_KINDS = 6


def chip_ring(side):
    order = list(range(side))
    for y in range(1, side):
        columns = range(1, side)
        order += [y * side + x for x in (reversed(columns) if y % 2 else columns)]
    order += [y * side for y in range(side - 1, 0, -1)]
    return order


def dot(left, right):
    return jnp.dot(left, right, preferred_element_type=F32)


def silu(values):
    half = 0.5 * values
    return half + half * jnp.tanh(half)


def layer_norm(values):
    centred = values - jnp.mean(values, axis=-1, keepdims=True)
    spread = jnp.mean(centred * centred, axis=-1, keepdims=True)
    return centred * lax.rsqrt(spread + 1e-5)


def tail(pre_act, w_second):
    return layer_norm(dot(silu(pre_act).astype(BF16), w_second))


def pick(index, table):
    found = jnp.int32(0)
    for position, value in enumerate(table):
        found = found + jnp.where(index == position, jnp.int32(value), jnp.int32(0))
    return found


def rows_mod(shape, modulus):
    return lax.broadcasted_iota(jnp.int32, shape, 0) & (modulus - 1)


def next_quarter(values):
    rows = values.shape[0]
    return jnp.where(rows_mod(values.shape, 4) < 3, pltpu.roll(values, rows - 1, 0), pltpu.roll(values, 3, 0))


def prev_quarter(values):
    rows = values.shape[0]
    return jnp.where(rows_mod(values.shape, 4) > 0, pltpu.roll(values, 1, 0), pltpu.roll(values, rows - 3, 0))


def kernel(cfg, xp_h, xc_h, frc_in, fix_in, m2g_in, g2m_in, mef_in, mft_in, ns_in, wpad, wfin, wembed_h, win_h, wout_h, nin_h, nout_h, wself_h, whid_h,
           out_a, out_b,
           xbuf, tbuf, nat, mt, gf_in, mf_in, wembed, win, wout, nin, nout, wself, whid, state, perm, mf_next, mf_all, mf_blk,
           fst_s, fst_r, stage_s, stage_r, back_s, back_r, mesh_buf, halo,
           edges, edge_base, mesh_lat, g2m_lat, m2g_lat, grid_lat, grid_cur,
           enc_base, enc_node, dec_base, dec_static, dec_node, mesh_band,
           proj, recv, node_pre, acc, pre_ref, far,
           misc_sem, wl_sem, shift_sem, fst_ss, fst_rs, stg_ss, stg_rs, bck_ss, bck_rs, halo_ss, halo_rs):
    group, ring, latent, ratio, layers, half = cfg
    chips = len(ring)
    mesh_dev = 2 * half
    grid_dev = ratio * mesh_dev
    chunk = grid_dev // 2
    devices = [2 * ring[q // 2] + q % 2 for q in range(group)]
    me = lax.axis_index("gp")
    core = me % 2
    where_of = [0] * chips
    for position, chip in enumerate(ring):
        where_of[chip] = position
    chip_place = pick(me // 2, where_of)
    place = 2 * chip_place + core
    up = jnp.where(core == 0, me + 1, 2 * pick(chip_place, ring[1:] + ring[:1]))
    down = jnp.where(core == 1, me - 1, 2 * pick(chip_place, ring[-1:] + ring[:-1]) + 1)

    def target(index):
        return dict(device_id={"gp": index}, device_id_type=pl.DeviceIdType.MESH)

    def local(source, dest, sem):
        return pltpu.make_async_copy(source, dest, sem)

    def block_copies(block, slot):
        return [local(win_h.at[block], win.at[slot], wl_sem.at[slot, 0]), local(wout_h.at[block], wout.at[slot], wl_sem.at[slot, 1]),
                local(nin_h.at[block], nin.at[slot], wl_sem.at[slot, 2]), local(nout_h.at[block], nout.at[slot], wl_sem.at[slot, 3])]

    x_copies = [local(xp_h, xbuf.at[0], misc_sem.at[3]), local(xc_h, xbuf.at[1], misc_sem.at[4])]
    embed_copy = local(wembed_h, wembed, misc_sem.at[0])
    self_copy = local(wself_h, wself, misc_sem.at[1])
    hid_copy = local(whid_h, whid, misc_sem.at[2])
    enc_copies = block_copies(0, 2)
    dec_copies = block_copies(layers + 1, 3)
    for copy in [embed_copy] + x_copies + enc_copies + [self_copy] + dec_copies + [hid_copy] + block_copies(1, 0):
        copy.start()

    barrier = pltpu.get_barrier_semaphore()
    for hop in range(1, group):
        pl.semaphore_signal(barrier, inc=1, **target(lax.rem(me + hop, group)))

    row = lax.broadcasted_iota(jnp.int32, (mesh_dev, mesh_dev), 0)
    col = lax.broadcasted_iota(jnp.int32, (mesh_dev, mesh_dev), 1)

    def by_target(index):
        return ((index >> 1) & 1) * half + (index >> 2) * 2 + (index & 1)

    def by_source(index):
        b = (index >> 2) & 15
        return ((index & 3) * 8 + (b >> 1)) * 4 + (b & 1) * 2 + (index >> 6)

    for slot, mask in enumerate((by_target(row) == col, by_source(row) == col, row == by_source(col), row == by_target(col))):
        perm[slot] = jnp.where(mask, 1.0, 0.0).astype(BF16)

    for ref in (enc_base, enc_node, dec_base, dec_node, dec_static, acc, proj, recv, node_pre, pre_ref, far, state, tbuf, mt):
        ref[...] = jnp.zeros_like(ref)
    def halves():
        return [(part * chunk, (part + 1) * chunk) for part in range(2)]

    steps, force = frc_in.shape[1], frc_in.shape[0]
    fixed, efeat = fix_in.shape[0], m2g_in.shape[0]
    for f in range(force):
        for which in range(steps):
            tbuf[which * force + f:which * force + f + 1] = frc_in[f, which:which + 1]
    at = steps * force
    tbuf[at:at + fixed] = fix_in[...]
    at += fixed
    tbuf[at:at + efeat] = m2g_in[...]
    at += efeat
    tbuf[at:at + efeat] = g2m_in[...]
    nat[...] = tbuf[...].T
    for k in range(EDGE_KINDS):
        mt[k * efeat:(k + 1) * efeat] = mef_in[k]
    base = EDGE_KINDS * efeat
    mt[base:base + mft_in.shape[0]] = mft_in[...]
    base += mft_in.shape[0]
    turned = mt[...].T
    lane = lax.broadcasted_iota(jnp.int32, turned.shape, 1)
    for r in range(ratio):
        rows = nat[pl.ds(r, mesh_dev, stride=ratio), :]
        gf_in[r * mesh_dev:(r + 1) * mesh_dev] = rows.astype(BF16)
        first = base + r * efeat
        turned = jnp.where(jnp.logical_and(lane >= first, lane < first + efeat), pltpu.roll(rows, first - at, 1), turned)
    mf_in[...] = turned.astype(BF16)
    tbuf[...] = jnp.zeros_like(tbuf)
    embed_copy.wait()
    for lo, hi in halves()[:1]:
        m2g_lat[lo:hi] = tail(dot(gf_in[lo:hi], wpad[4]), wembed[3]).astype(BF16)
    pl.semaphore_wait(barrier, group - 1)
    shift = pltpu.make_async_remote_copy(mf_in.at[pl.ds(0, half)], mf_next, shift_sem.at[0], shift_sem.at[1],
                                         **target(lax.rem(me + group - 1, group)))
    shift.start()

    def exchange(src, dst, send_sem, recv_sem, slot, dest_of, source_of):
        copies = []
        for part in range(group):
            dest = dest_of(part)
            copy = pltpu.make_async_remote_copy(src.at[part], dst.at[slot], send_sem.at[part], recv_sem.at[slot], **target(dest))
            copies.append((dest, copy))

            @pl.when(dest != me)
            def _(copy=copy):
                copy.start()

            @pl.when(dest == me)
            def _(part=part):
                dst[slot] = src[part]

        def finish():
            for part in range(group):
                @pl.when(source_of(part) != me)
                def _(part=part):
                    pltpu.make_async_remote_copy(src.at[part], dst.at[part], send_sem.at[part], recv_sem.at[part], **target(up)).wait_recv()

            for dest, copy in copies:
                @pl.when(dest != me)
                def _(copy=copy):
                    copy.wait_send()
        return finish

    def forth(src, dst, send_sem, recv_sem):
        return exchange(src, dst, send_sem, recv_sem, me, lambda q: devices[q], lambda d: d)

    def back(src, dst, send_sem, recv_sem):
        return exchange(src, dst, send_sem, recv_sem, place, lambda d: d, lambda q: devices[q])

    for lo, hi in halves()[1:]:
        m2g_lat[lo:hi] = tail(dot(gf_in[lo:hi], wpad[4]), wembed[3]).astype(BF16)
    for copy in x_copies:
        copy.wait()
    for which in range(2):
        tbuf[:xbuf.shape[1]] = xbuf[which]
        nat[...] = tbuf[...].T
        for r in range(ratio):
            state[which, r * mesh_dev:(r + 1) * mesh_dev] = nat[pl.ds(r, mesh_dev, stride=ratio), :]
    shift.wait()
    mf_all[:half] = mf_in[half:]
    mf_all[half:] = mf_next[...]
    feats = mf_all[...]
    fst_s[...] = dot(perm[0], feats).astype(BF16).reshape(fst_s.shape)
    fst_done = forth(fst_s, fst_r, fst_ss, fst_rs)
    mesh_lat[...] = tail(dot(feats, wpad[5 + EDGE_KINDS]), wembed[1]).astype(BF16)
    for copy in enc_copies:
        copy.wait()
    recv[...] = dot(mesh_lat[...], win[2, 2 * latent:])
    enc_node[...] = dot(mesh_lat[...], nin[2, :latent])
    for r in range(ratio):
        dec_base[r * mesh_dev:(r + 1) * mesh_dev] = dot(feats, wpad[6 + EDGE_KINDS + r])
    for lo, hi in halves():
        g2m_lat[lo:hi] = tail(dec_base[lo:hi], wembed[2]).astype(BF16)
    for lo, hi in halves():
        dec_node[lo:hi] = dot(g2m_lat[lo:hi], win[2, :latent])
    for r in range(ratio):
        rows = slice(r * mesh_dev, (r + 1) * mesh_dev)
        enc_base[rows] = dec_node[rows] + recv[...]
    for copy in dec_copies:
        copy.wait()
    for lo, hi in halves():
        dec_static[lo:hi] = dot(m2g_lat[lo:hi], win[3, :latent])
    self_copy.wait()
    hid_copy.wait()

    top, low_end = 4 * mesh_dev, 5 * mesh_dev
    near_index, far_index = core, 1 - core
    low = lax.broadcasted_iota(jnp.int32, (8, latent), 0) < 4

    def step_up(values):
        moved = pltpu.roll(values, half - 4, 0)
        last = moved[half - 8:]
        return jnp.concatenate([moved[:half - 8], jnp.where(low, last, next_quarter(last))], axis=0)

    def step_down(values):
        moved = pltpu.roll(values, 4, 0)
        first = moved[:8]
        return jnp.concatenate([jnp.where(low, prev_quarter(first), first), moved[8:]], axis=0)

    def run_layer(step, layer):
        slot = layer % 2
        later = 1 - slot

        def send(part, dest):
            return pltpu.make_async_remote_copy(mesh_buf.at[slot, pl.ds(part * half, half)], halo.at[slot, part],
                                                halo_ss.at[slot, part], halo_rs.at[slot, part], **target(dest))
        to_down, to_up = send(0, down), send(1, up)

        @pl.when(core == 0)
        def _():
            to_down.start()
            to_up.start()

        @pl.when(core == 1)
        def _():
            to_up.start()
            to_down.start()

        for copy in block_copies(layer + 1, slot):
            copy.wait()

        @pl.when(jnp.logical_or(step == 0, layer < layers - 1))
        def _():
            for copy in block_copies(1 + (layer + 1) % layers, later):
                copy.start()

        @pl.when(layer == 0)
        def _():
            edges[...] = edge_base[...]

        w_edge = win.at[slot]
        w_edge_two = wout.at[slot]
        w_node = nin.at[slot]
        w_node_two = nout.at[slot]
        nodes = mesh_buf[slot]
        proj[...] = dot(nodes, w_edge[latent:2 * latent])
        recv[...] = dot(nodes, w_edge[2 * latent:])
        pre_ref[...] = dot(edges[...], w_edge[:latent])

        def renew(lo, rows, sent):
            hidden = silu(pre_ref[lo:lo + sent.shape[0]] + sent + rows).astype(BF16)
            return hidden

        everyone = recv[...]
        hidden_a = jnp.concatenate([
            renew(2 * mesh_dev, everyone, next_quarter(proj[...])),
            renew(3 * mesh_dev, everyone, prev_quarter(proj[...])),
            renew(top, everyone, jnp.concatenate([proj[half:], proj[:half]], axis=0))], axis=0)
        out_a_rows = dot(hidden_a, w_edge_two[...])
        hidden_b = jnp.concatenate([
            renew(0, everyone, jnp.concatenate([step_up(proj[:half]), step_up(proj[half:])], axis=0)),
            renew(mesh_dev, everyone, jnp.concatenate([step_down(proj[:half]), step_down(proj[half:])], axis=0))], axis=0)
        out_b_rows = dot(hidden_b, w_edge_two[...])
        node_pre[...] = dot(nodes, w_node[:latent])

        def settle(lo, values, first=False):
            new = (edges[lo:lo + mesh_dev].astype(F32) + layer_norm(values)).astype(BF16)
            edges[lo:lo + mesh_dev] = new
            acc[...] = new.astype(F32) if first else acc[...] + new.astype(F32)

        settle(2 * mesh_dev, out_a_rows[:mesh_dev], first=True)
        settle(3 * mesh_dev, out_a_rows[mesh_dev:2 * mesh_dev])
        settle(top, out_a_rows[2 * mesh_dev:])
        settle(0, out_b_rows[:mesh_dev])
        settle(mesh_dev, out_b_rows[mesh_dev:])

        def side(index, sent):
            lo = pl.multiple_of(low_end + index * half, half)
            into = pl.multiple_of((1 - index) * half, half)
            pre = pre_ref[pl.ds(lo, half)] + sent + recv[pl.ds(into, half)]
            new = (edges[pl.ds(lo, half)].astype(F32) + tail(pre, w_edge_two[...])).astype(BF16)
            edges[pl.ds(lo, half)] = new
            acc[pl.ds(into, half)] = acc[pl.ds(into, half)] + new.astype(F32)

        def arrived(index):
            pltpu.make_async_remote_copy(mesh_buf.at[slot, pl.ds(0, half)], halo.at[slot, index],
                                         halo_ss.at[slot, index], halo_rs.at[slot, index], **target(up)).wait_recv()

        arrived(near_index)
        far[...] = dot(halo[slot, near_index], w_edge[latent:2 * latent])
        side(near_index, far[...])
        arrived(far_index)
        far[...] = dot(halo[slot, far_index], w_edge[latent:2 * latent])
        sent = far[...]
        sent = jnp.where(place == group - 1, step_up(sent), jnp.where(place == 0, step_down(sent), sent))
        side(far_index, sent)
        update = tail(node_pre[...] + dot(acc[...].astype(BF16), w_node[latent:]), w_node_two[...])
        to_down.wait_send()
        to_up.wait_send()
        mesh_buf[later] = (nodes.astype(F32) + update).astype(BF16)

    mean, spread, diff_mean, diff_spread = ns_in[0:1], ns_in[1:2], ns_in[2:3], ns_in[3:4]

    def run_step(step):
        after = lax.rem(step + 2, 3)
        for lo, hi in halves():
            past = ((state[step, lo:hi] - mean) / spread).astype(BF16)
            now = ((state[step + 1, lo:hi] - mean) / spread).astype(BF16)
            pre = dot(past, wpad[0]) + dot(now, wpad[1]) + dot(gf_in[lo:hi], wpad[2 + step])
            grid_lat[lo:hi] = tail(pre, wembed[0]).astype(BF16)
        for part, (lo, hi) in enumerate(halves()):
            pre = enc_base[lo:hi] + dot(grid_lat[lo:hi], win[2, latent:2 * latent])
            new = (g2m_lat[lo:hi].astype(F32) + tail(pre, wout[2])).astype(BF16).astype(F32)
            total = new[:mesh_dev] + new[mesh_dev:]
            acc[...] = total if part == 0 else acc[...] + total
        update = tail(enc_node[...] + dot(acc[...].astype(BF16), nin[2, latent:]), nout[2])
        mesh_band[...] = (mesh_lat[...].astype(F32) + update).astype(BF16)
        stage_s[...] = dot(perm[0], mesh_band[...]).astype(BF16).reshape(stage_s.shape)
        arrive = forth(stage_s, stage_r, stg_ss, stg_rs)
        for lo, hi in halves():
            lat = grid_lat[lo:hi]
            grid_cur[lo:hi] = (lat.astype(F32) + tail(dot(lat, wself[0]), wself[1])).astype(BF16)

        @pl.when(step == 0)
        def _():
            fst_done()
            mf_blk[...] = dot(perm[1], fst_r[...].reshape(mesh_dev, LANES)).astype(BF16)
            for k in range(2, EDGE_KINDS):
                pre_ref[(k - 2) * mesh_dev:(k - 1) * mesh_dev] = dot(mf_blk[...], wpad[5 + k])
            pre_ref[top:top + half] = dot(mf_blk[:half], wpad[5])
            pre_ref[top + half:low_end] = dot(mf_blk[half:], wpad[6])
            pre_ref[low_end:low_end + half] = dot(mf_blk[half:], wpad[5])
            pre_ref[low_end + half:] = dot(mf_blk[:half], wpad[6])
            for lo in range(0, EDGE_KINDS * mesh_dev, chunk):
                edge_base[lo:lo + chunk] = tail(pre_ref[lo:lo + chunk], wembed[4]).astype(BF16)

        arrive()
        mesh_buf[0] = dot(perm[1], stage_r[...].reshape(mesh_dev, latent)).astype(BF16)

        @pl.loop(0, layers)
        def _(layer):
            run_layer(step, layer)

        back_s[...] = dot(perm[2], mesh_buf[layers % 2]).astype(BF16).reshape(back_s.shape)
        arrive = back(back_s, back_r, bck_ss, bck_rs)
        for lo, hi in halves():
            dec_base[lo:hi] = dec_static[lo:hi] + dot(grid_cur[lo:hi], win[3, 2 * latent:])
            dec_node[lo:hi] = dot(grid_cur[lo:hi], nin[3, :latent])
        arrive()
        mesh_band[...] = dot(perm[3], back_r[...].reshape(mesh_dev, latent)).astype(BF16)
        recv[...] = dot(mesh_band[...], win[3, latent:2 * latent])
        for lo, hi in halves():
            pre = dec_base[lo:hi] + jnp.concatenate([recv[...], recv[...]], axis=0)
            dec_edge = (m2g_lat[lo:hi].astype(F32) + tail(pre, wout[3])).astype(BF16)
            update = tail(dec_node[lo:hi] + dot(dec_edge, nin[3, latent:]), nout[3])
            grid_out = (grid_cur[lo:hi].astype(F32) + update).astype(BF16)
            hidden = silu(dot(grid_out, whid[...])).astype(BF16)
            state[after, lo:hi] = state[step + 1, lo:hi] + diff_spread * lax.dot_general(hidden, wfin[...], (((1,), (1,)), ((), ())), preferred_element_type=F32) + diff_mean
        for r in range(ratio):
            nat[pl.ds(r, mesh_dev, stride=ratio), :] = state[after, r * mesh_dev:(r + 1) * mesh_dev]
        tbuf[...] = nat[...].T

        @pl.when(step == 0)
        def _():
            out_a[...] = tbuf[:out_a.shape[0]]

        @pl.when(step == 1)
        def _():
            out_b[...] = tbuf[:out_b.shape[0]]

    @pl.loop(0, 2)
    def _(step):
        run_step(step)


def solution(mesh):
    group = mesh.shape["gp"]
    side = math.isqrt(group // 2)
    ring = chip_ring(side)
    row_spec = P(("dp", "gp"))
    edge_spec = P(("dp", "gp"), None, None)
    whole = P()

    def local_run(x_prev, x_cur, forcing, grid_static, g2m_feat, m2g_feat, mesh_feat, mesh_edge_feat, norm_stats, w_grid_in, w_mesh_in, w_eemb_in, w_embed_out, w_edge_in, w_edge_out, w_node_in, w_node_out, w_grid_self, w_out_hidden, w_out_final):
        grid_dev, variables = x_prev.shape
        mesh_dev = mesh_feat.shape[0]
        ratio = grid_dev // mesh_dev
        latent = w_embed_out.shape[-1]
        layers = w_edge_in.shape[0] - 2
        steps, force = forcing.shape[1:]
        fixed = grid_static.shape[1]
        efeat = m2g_feat.shape[1]
        assert side * side * 2 == group and mesh_dev == 8 * len(ring) and mesh_dev == 128 and ratio == 4 and layers % 2 == 0

        def lanes(values, fill=0):
            return jnp.pad(values, [(0, 0)] * (values.ndim - 1) + [(0, LANES - values.shape[-1])], constant_values=fill)

        kinds = mesh_edge_feat.shape[1]
        ns = jnp.stack([lanes(norm_stats[0]), lanes(norm_stats[1], 1), lanes(norm_stats[2]), lanes(norm_stats[3])])

        def placed(*pieces):
            total = 0
            for start, rows in pieces:
                total = total + jnp.pad(rows, ((start, LANES - start - rows.shape[0]), (0, 0)))
            return total

        w_force = w_grid_in[2 * variables:2 * variables + force]
        w_fixed = w_grid_in[2 * variables + force:]
        start = steps * force
        pads = [placed((0, w_grid_in[:variables])), placed((0, w_grid_in[variables:2 * variables])),
                placed((0, w_force), (start, w_fixed)), placed((force, w_force), (start, w_fixed)),
                placed((start + fixed, w_eemb_in[1]))]
        pads += [placed((k * efeat, w_eemb_in[2])) for k in range(kinds)]
        pads += [placed((kinds * efeat, w_mesh_in))]
        pads += [placed((kinds * efeat + mesh_feat.shape[1] + r * efeat, w_eemb_in[0])) for r in range(ratio)]
        wpad = jnp.stack(pads)
        wfin = jnp.pad(w_out_final.T, ((0, LANES - variables), (0, 0)))

        vmem = pl.BlockSpec(memory_space=pltpu.VMEM)
        hbm = pl.BlockSpec(memory_space=pl.ANY)
        VM = pltpu.VMEM
        DMA = pltpu.SemaphoreType.DMA
        grid_shape = (grid_dev, latent)
        node_shape = (mesh_dev, latent)
        part_shape = (group, mesh_dev // group, latent)
        feat_shape = part_shape[:2] + (LANES,)
        edge_shape = (EDGE_KINDS * mesh_dev, latent)
        half = mesh_dev // 2
        scratch = [
            VM((2, variables, grid_dev), F32), VM((LANES, grid_dev), F32), VM((grid_dev, LANES), F32), VM((LANES, mesh_dev), F32), VM((grid_dev, LANES), BF16), VM((mesh_dev, LANES), BF16),
            VM(w_embed_out.shape, BF16), VM((4,) + w_edge_in.shape[1:], BF16), VM((4,) + w_edge_out.shape[1:], BF16),
            VM((4,) + w_node_in.shape[1:], BF16), VM((4,) + w_node_out.shape[1:], BF16), VM(w_grid_self.shape, BF16), VM(w_out_hidden.shape, BF16),
            VM((3, grid_dev, LANES), F32), VM((4, mesh_dev, mesh_dev), BF16),
            VM((half, LANES), BF16), VM((mesh_dev, LANES), BF16), VM((mesh_dev, LANES), BF16),
            VM(feat_shape, BF16), VM(feat_shape, BF16), VM(part_shape, BF16), VM(part_shape, BF16), VM(part_shape, BF16), VM(part_shape, BF16),
            VM((2,) + node_shape, BF16), VM((2, 2, half, latent), BF16),
            VM(edge_shape, BF16), VM(edge_shape, BF16), VM(node_shape, BF16),
            VM(grid_shape, BF16), VM(grid_shape, BF16), VM(grid_shape, BF16), VM(grid_shape, BF16),
            VM(grid_shape, F32), VM(node_shape, F32), VM(grid_shape, F32), VM(grid_shape, F32), VM(grid_shape, F32), VM(node_shape, BF16),
            VM(node_shape, F32), VM(node_shape, F32), VM(node_shape, F32), VM(node_shape, F32), VM(edge_shape, F32), VM((half, latent), F32),
            DMA((5,)), DMA((4, 4)), DMA((2,)), DMA((group,)), DMA((group,)), DMA((group,)), DMA((group,)), DMA((group,)), DMA((group,)), DMA((2, 2)), DMA((2, 2)),
        ]
        cfg = (group, ring, latent, ratio, layers, mesh_dev // 2)
        next_t, after_t = pl.pallas_call(
            functools.partial(kernel, cfg),
            out_shape=(jax.ShapeDtypeStruct((variables, grid_dev), F32),) * 2,
            in_specs=[hbm] * 2 + [vmem] * 9 + [hbm] * 7,
            out_specs=(vmem, vmem),
            scratch_shapes=scratch,
            compiler_params=pltpu.CompilerParams(collective_id=0, has_side_effects=True, vmem_limit_bytes=60 * 1024 * 1024),
        )(x_prev.T, x_cur.T, forcing.transpose(2, 1, 0), grid_static.T, m2g_feat.T, g2m_feat.T, mesh_edge_feat.transpose(1, 2, 0), mesh_feat.T, ns, wpad, wfin,
          w_embed_out, w_edge_in, w_edge_out, w_node_in, w_node_out, w_grid_self, w_out_hidden)
        return next_t.T, after_t.T

    in_specs = (row_spec, row_spec, edge_spec, row_spec, row_spec, row_spec, row_spec, edge_spec, whole) + (whole,) * 11
    return jax.shard_map(local_run, mesh=mesh, in_specs=in_specs, out_specs=(row_spec, row_spec), check_vma=False)
```
